32 devices in a mesh: tok: 4 (over y, x), din: 4 (over z), dout: 2 (over core).
Axes of the slice: x: 2, y: 2, z: 4, core: 2. Of those that a mesh axis runs over, the one named last changes fastest.
Arguments:
- inputs: bfloat16 [1024, 7168], P(('tok', 'dout'), 'din'), may hold values from -6 to 6
- out_grad: bfloat16 [1024, 9216], P(('tok', 'din'), 'dout'), may hold values from -0.1875 to 0.1875
Outputs:
- weight_grad: bfloat16 [7168, 9216], P(('din', 'tok'), 'dout')
The draws below stay inside these ranges and needn't reach their ends.
All inputs are finite; a program needn't handle non-finite values.
Results may differ from the reference program's by a relative error of at most 0.014.
Values may be sent and summed in bfloat16 or wider, within the bound.
A program may use at most 64 MiB of HBM per device.

```python
import jax
import jax.numpy as jnp
from jax import lax

D = 7168
F = 9216
GROUP_ROWS = 256
TOKENS = 1024
N_TOK = 4


def spiked(drawn, rng, source, target, shards_of, factor):
    def block_of(axis_at):
        return (jnp.arange(drawn.shape[axis_at]) // (drawn.shape[axis_at] // shards_of)).reshape((-1,) + (1,) * (drawn.ndim - 1 - axis_at))

    near = jax.random.permutation(rng, shards_of)[block_of(target)]
    other_side = (block_of(target) + shards_of // 2) % shards_of
    return jnp.where((block_of(source) == near) | (block_of(source) == other_side), factor * drawn, drawn)


def block_levels(key, extent, split, smallest, largest):
    def one(position, parts):
        heights = jax.random.uniform(jax.random.fold_in(jax.random.fold_in(key, 6), position), (parts,), jnp.float32, smallest / len(split), largest / len(split))
        return jnp.repeat(jnp.exp(heights), extent[position] // parts).reshape((-1,) + (1,) * (len(extent) - position - 1))

    loudness = one(*split[0])
    for cut in split[1:]:
        loudness = loudness * one(*cut)
    return loudness


def gaussian(key, extent, scale, limit, split=(), kind=jnp.bfloat16):
    drawn = scale * jax.random.normal(key, extent, jnp.float32)
    if split:
        drawn = drawn * block_levels(key, extent, split, -0.22, 0.18)
    return jnp.clip(drawn, -limit, limit).astype(kind)


def noise_with(stream_key, dims, spread, reach, cuts, heavy, kind=jnp.bfloat16):
    result = spread * jax.random.normal(stream_key, dims, jnp.float32)
    if cuts:
        result = result * block_levels(stream_key, dims, cuts, -0.22, 0.18)
    return jnp.clip(spiked(result, jax.random.fold_in(stream_key, 3), *heavy), -reach, reach).astype(kind)


def setup_inputs(seed: int = 0) -> dict:
    seeds = jax.random.split(jax.random.key(seed), 3)
    inputs = noise_with(seeds[0], (TOKENS, D), 1.0, 6.0, ((0, 8), (1, 4)), (0, 1, 8, 2.0))
    out_grad = gaussian(seeds[1], (TOKENS, F), TOKENS ** -0.5, 0.1875, ((0, 16), (1, 2)))
    return {"inputs": inputs, "out_grad": out_grad}


def reference(inputs, out_grad):
    def add_group(total, index):
        start = (index * GROUP_ROWS).astype(jnp.int32)
        rows_in = lax.dynamic_slice_in_dim(inputs, start, GROUP_ROWS, 0)
        rows_grad = lax.dynamic_slice_in_dim(out_grad, start, GROUP_ROWS, 0)
        term = lax.dot_general(rows_in, rows_grad, (((0,), (0,)), ((), ())), preferred_element_type=jnp.float32)
        return total + term.astype(jnp.bfloat16).astype(jnp.float32), None

    total = jnp.zeros((D, F), jnp.float32)
    total, _ = lax.scan(add_group, total, jnp.arange(N_TOK, dtype=jnp.int32))
    return total.astype(jnp.bfloat16)
```

```python
import functools

import jax
import jax.numpy as jnp
from jax import lax
from jax.experimental import pallas as pl
from jax.experimental.pallas import tpu as pltpu
from jax.sharding import PartitionSpec as P

MESH = pl.DeviceIdType.MESH
LANES = 128
KINDS = 4


def scattered(inputs, out_grad):
    gathered = lax.all_gather(inputs, "dout", axis=0, tiled=True)
    partial_term = lax.dot_general(
        gathered,
        lax.all_gather(out_grad, "din", axis=0, tiled=True),
        (((0,), (0,)), ((), ())),
        preferred_element_type=jnp.float32,
    )
    return lax.psum_scatter(
        partial_term.astype(jnp.bfloat16), "tok", scatter_dimension=0, tiled=True
    )


def kernel(sizes, a_ref, g_ref, o_ref, held, windows, turned, left, made,
           load_sem, a_load, a_send, a_recv, a_pass, a_got, z_send, z_recv, p_send, p_recv, o_sem):
    depth, chunks, rows, window = sizes
    t, z, core = lax.axis_index("tok"), lax.axis_index("din"), lax.axis_index("dout")
    y, x = t // 2, t % 2
    tx, ty = y * 2 + (1 - x), (1 - y) * 2 + x
    td = (1 - y) * 2 + (1 - x)
    wide = KINDS * LANES

    def at_t(other):
        return (other, z, core)

    partner = (t, z, 1 - core)

    def own(c, k):
        return pltpu.make_async_copy(
            g_ref.at[:, pl.ds(pl.multiple_of(c * wide + k * LANES, LANES), LANES)],
            held.at[c, k, y, x, z],
            load_sem.at[c, k],
        )

    def load(c, carry):
        for k in range(KINDS):
            own(c, k).start()
        return carry

    lax.fori_loop(0, chunks, load, 0)

    barrier = pltpu.get_barrier_semaphore()
    for other in (at_t(tx), at_t(ty), at_t(td), partner):
        pl.semaphore_signal(barrier, inc=1, device_id=other, device_id_type=MESH)

    @pl.when(z > 0)
    def _():
        pl.semaphore_signal(barrier, inc=1, device_id=(t, z - 1, core), device_id_type=MESH)

    @pl.when(z < depth - 1)
    def _():
        pl.semaphore_signal(barrier, inc=1, device_id=(t, z + 1, core), device_id_type=MESH)

    pl.semaphore_wait(barrier, 4 + jnp.where(z > 0, 1, 0) + jnp.where(z < depth - 1, 1, 0))

    def slab(owner):
        start = pl.multiple_of((owner * rows) // LANES * LANES, LANES)
        return a_ref.at[:, pl.ds(start, window)]

    def a_copy(j, target):
        return pltpu.make_async_remote_copy(
            src_ref=slab(target), dst_ref=windows.at[t, core],
            send_sem=a_send.at[j], recv_sem=a_recv.at[j],
            device_id=at_t(target), device_id_type=MESH,
        )

    def a_wait(j, source):
        pltpu.make_async_remote_copy(
            src_ref=slab(source), dst_ref=windows.at[source, core],
            send_sem=a_send.at[j], recv_sem=a_recv.at[j],
            device_id=at_t(source), device_id_type=MESH,
        ).wait_recv()

    def a_over(j, source, src):
        return pltpu.make_async_remote_copy(
            src_ref=src, dst_ref=windows.at[source, core],
            send_sem=a_pass.at[j], recv_sem=a_got.at[j],
            device_id=partner, device_id_type=MESH,
        )

    def a_over_wait(j, source):
        pltpu.make_async_remote_copy(
            src_ref=windows.at[source, 1 - core], dst_ref=windows.at[source, 1 - core],
            send_sem=a_pass.at[j], recv_sem=a_got.at[j],
            device_id=partner, device_id_type=MESH,
        ).wait_recv()

    mine = pltpu.make_async_copy(slab(t), windows.at[t, core], a_load)
    mine.start()

    def plane_ref(c, k, last, yy, xx):
        if k == 0:
            return held.at[c, k, yy] if last else held.at[c, k, yy, xx]
        if k == 1:
            return held.at[c, k, :, xx] if last else held.at[c, k, yy, xx]
        if not last:
            return held.at[c, k, yy, xx, z]
        return held.at[c, k, yy] if k == 2 else held.at[c, k, :, xx]

    def along_x(k, last):
        return (k in (0, 2)) != last

    def plane(c, k, last):
        ref = plane_ref(c, k, last, y, x)
        return pltpu.make_async_remote_copy(
            src_ref=ref, dst_ref=ref,
            send_sem=p_send.at[c, k, int(last)], recv_sem=p_recv.at[c, k, int(last)],
            device_id=at_t(tx if along_x(k, last) else ty), device_id_type=MESH,
        )

    def plane_wait(c, k, last):
        yy, xx = (y, 1 - x) if along_x(k, last) else (1 - y, x)
        ref = plane_ref(c, k, last, yy, xx)
        pltpu.make_async_remote_copy(
            src_ref=ref, dst_ref=ref,
            send_sem=p_send.at[c, k, int(last)], recv_sem=p_recv.at[c, k, int(last)],
            device_id=at_t(tx if along_x(k, last) else ty), device_id_type=MESH,
        ).wait_recv()

    def line_ref(c, g, source):
        if g == 0:
            return held.at[c, pl.ds(0, 2), y, x, source]
        return held.at[c, 2, y, :, source] if g == 1 else held.at[c, 3, :, x, source]

    def line(c, g, source, up):
        ref = line_ref(c, g, source)
        return pltpu.make_async_remote_copy(
            src_ref=ref, dst_ref=ref,
            send_sem=z_send.at[c, g, source, up], recv_sem=z_recv.at[c, g, source],
            device_id=(t, z + 1 if up else z - 1, core), device_id_type=MESH,
        )

    def both_ways(c, g):
        @pl.when(z < depth - 1)
        def _():
            line(c, g, z, 1).start()

        @pl.when(z > 0)
        def _():
            line(c, g, z, 0).start()

    def first(c, carry):
        for k in range(KINDS):
            own(c, k).wait()
        for k in (2, 3):
            plane(c, k, False).start()
        return carry

    def send_own(c):
        both_ways(c, 0)
        for k in (2, 3):
            plane_wait(c, k, False)
            both_ways(c, k - 1)

    def pass_on(c):
        for hop in range(1, depth):
            for g in range(3):
                @pl.when(z - hop >= 0)
                def _():
                    line(c, g, z - hop, 0).wait_recv()

                    @pl.when(z < depth - 1)
                    def _():
                        line(c, g, z - hop, 1).start()

                @pl.when(z + hop < depth)
                def _():
                    line(c, g, z + hop, 1).wait_recv()

                    @pl.when(z > 0)
                    def _():
                        line(c, g, z + hop, 0).start()
        for k in (0, 1):
            plane(c, k, False).start()
        for k in (2, 3):
            plane(c, k, True).start()

    def finish(c):
        for k in (0, 1):
            plane_wait(c, k, False)
            plane(c, k, True).start()

    def out_copy(c):
        return pltpu.make_async_copy(
            made.at[c], o_ref.at[:, pl.ds(pl.multiple_of(c * wide, LANES), wide)], o_sem.at[c]
        )

    def multiply(c):
        for k in range(KINDS):
            plane_wait(c, k, True)
        for k in range(0, KINDS, 2):
            pair = [held[c, k + i].reshape(-1, LANES) for i in range(2)]
            term = jnp.dot(
                left[...], jnp.concatenate(pair, axis=1), preferred_element_type=jnp.float32
            )
            made[c, :, k * LANES:(k + 2) * LANES] = term.astype(made.dtype)
        out_copy(c).start()

    first(0, 0)
    for j, target in enumerate((tx, ty, td)):
        a_copy(j, target).start()
    a_over(3, t, slab(t)).start()
    both_ways(0, 0)
    lax.fori_loop(1, chunks, first, 0)
    for k in (2, 3):
        plane_wait(0, k, False)
        both_ways(0, k - 1)

    mine.wait()
    for j, source in enumerate((tx, ty, td)):
        a_wait(j, source)
        a_over(j, source, windows.at[source, core]).start()
    for j, source in enumerate((tx, ty, td, t)):
        a_over_wait(j, source)
    shift = pl.multiple_of((t * rows) % LANES, 16)

    count = windows.shape[0] * 2
    for j in range(count):
        turned[...] = windows[j // 2, j % 2].T
        piece = windows.shape[2]
        left[:, j * piece:(j + 1) * piece] = turned[pl.ds(shift, rows), :]

    def step(i, carry):
        @pl.when(i + 1 < chunks)
        def _():
            send_own(i + 1)

        @pl.when(i < chunks)
        def _():
            pass_on(i)

        @pl.when((i >= 1) & (i < chunks + 1))
        def _():
            finish(i - 1)

        @pl.when(i >= 2)
        def _():
            multiply(i - 2)

        return carry

    lax.fori_loop(0, chunks + 2, step, 0)

    for j, target in enumerate((tx, ty, td)):
        a_copy(j, target).wait_send()
        a_over(j, target, windows.at[target, core]).wait_send()
    a_over(3, t, slab(t)).wait_send()

    def drain(c, carry):
        for k in range(KINDS):
            for last in (False, True):
                plane(c, k, last).wait_send()
        for g in range(3):
            for source in range(depth):
                @pl.when((z < depth - 1) & (z >= source))
                def _():
                    line(c, g, source, 1).wait_send()

                @pl.when((z > 0) & (z <= source))
                def _():
                    line(c, g, source, 0).wait_send()
        out_copy(c).wait()
        return carry

    lax.fori_loop(0, chunks, drain, 0)


def gathered(shape, inputs, out_grad):
    depth = shape["din"]
    groups = shape["tok"]
    rows = inputs.shape[1] // groups
    window = max((j * rows) % LANES for j in range(groups)) + rows
    window = -(-window // LANES) * LANES
    piece = inputs.shape[0]
    tall, columns = out_grad.shape
    wide = KINDS * LANES
    chunks = columns // wide
    tokens = tall * depth * groups
    any_ref = pl.BlockSpec(memory_space=pl.ANY)
    dma = pltpu.SemaphoreType.DMA
    return pl.pallas_call(
        functools.partial(kernel, (depth, chunks, rows, window)),
        out_shape=jax.ShapeDtypeStruct((rows, columns), out_grad.dtype),
        in_specs=[any_ref, any_ref],
        out_specs=any_ref,
        scratch_shapes=[
            pltpu.VMEM((chunks, KINDS, 2, 2, depth, tall, LANES), out_grad.dtype),
            pltpu.VMEM((groups, 2, piece, window), inputs.dtype),
            pltpu.VMEM((window, piece), inputs.dtype),
            pltpu.VMEM((rows, tokens), inputs.dtype),
            pltpu.VMEM((chunks, rows, wide), out_grad.dtype),
            dma((chunks, KINDS)),
            dma,
            dma((3,)),
            dma((3,)),
            dma((4,)),
            dma((4,)),
            dma((chunks, 3, depth, 2)),
            dma((chunks, 3, depth)),
            dma((chunks, KINDS, 2)),
            dma((chunks, KINDS, 2)),
            dma((chunks,)),
        ],
        compiler_params=pltpu.CompilerParams(collective_id=0, has_side_effects=True),
        cost_estimate=pl.CostEstimate(
            flops=2 * rows * tokens * columns,
            bytes_accessed=2 * rows * columns,
            transcendentals=0,
        ),
    )(inputs, out_grad)


def solution(mesh):
    shape = dict(mesh.shape)

    def local(inputs, out_grad):
        groups, depth = shape["tok"], shape["din"]
        rows = inputs.shape[1] // groups
        tall = out_grad.shape[0]
        spread = tall * (groups * depth - 1)
        summed = rows * (groups - 1) + tall * (depth - 1)
        fits = (
            groups == 4
            and shape["dout"] == 2
            and inputs.shape[0] == LANES
            and rows % 16 == 0
            and tall % 16 == 0
            and out_grad.shape[1] % (KINDS * LANES) == 0
        )
        if fits and spread < summed:
            return gathered(shape, inputs, out_grad)
        return scattered(inputs, out_grad)

    placed = (P(("tok", "dout"), "din"), P(("tok", "din"), "dout"))
    return jax.shard_map(
        local, mesh=mesh, in_specs=placed, out_specs=P(("din", "tok"), "dout"), check_vma=False
    )
```

```python
import functools

import jax
import jax.numpy as jnp
from jax import lax
from jax.experimental import pallas as pl
from jax.experimental.pallas import tpu as pltpu
from jax.sharding import PartitionSpec as P

MESH = pl.DeviceIdType.MESH
LANES = 128
KINDS = 4


def scattered(inputs, out_grad):
    gathered = lax.all_gather(inputs, "dout", axis=0, tiled=True)
    partial_term = lax.dot_general(
        gathered,
        lax.all_gather(out_grad, "din", axis=0, tiled=True),
        (((0,), (0,)), ((), ())),
        preferred_element_type=jnp.float32,
    )
    return lax.psum_scatter(
        partial_term.astype(jnp.bfloat16), "tok", scatter_dimension=0, tiled=True
    )


def kernel(sizes, a_ref, g_ref, o_ref, held, windows, turned, left, made,
           load_sem, a_load, a_send, a_recv, a_pass, a_got, z_send, z_recv, p_send, p_recv, o_sem):
    depth, chunks, rows, window = sizes
    t, z, core = lax.axis_index("tok"), lax.axis_index("din"), lax.axis_index("dout")
    y, x = t // 2, t % 2
    tx, ty = y * 2 + (1 - x), (1 - y) * 2 + x
    td = (1 - y) * 2 + (1 - x)
    wide = KINDS * LANES

    def at_t(other):
        return (other, z, core)

    partner = (t, z, 1 - core)

    def own(c, k):
        return pltpu.make_async_copy(
            g_ref.at[:, pl.ds(pl.multiple_of(c * wide + k * LANES, LANES), LANES)],
            held.at[c, k, y, x, z],
            load_sem.at[c, k],
        )

    def load(c, carry):
        for k in range(KINDS):
            own(c, k).start()
        return carry

    lax.fori_loop(0, chunks, load, 0)

    barrier = pltpu.get_barrier_semaphore()
    for other in (at_t(tx), at_t(ty), at_t(td), partner):
        pl.semaphore_signal(barrier, inc=1, device_id=other, device_id_type=MESH)

    @pl.when(z > 0)
    def _():
        pl.semaphore_signal(barrier, inc=1, device_id=(t, z - 1, core), device_id_type=MESH)

    @pl.when(z < depth - 1)
    def _():
        pl.semaphore_signal(barrier, inc=1, device_id=(t, z + 1, core), device_id_type=MESH)

    pl.semaphore_wait(barrier, 4 + jnp.where(z > 0, 1, 0) + jnp.where(z < depth - 1, 1, 0))

    def slab(owner):
        start = pl.multiple_of((owner * rows) // LANES * LANES, LANES)
        return a_ref.at[:, pl.ds(start, window)]

    def a_copy(j, target):
        return pltpu.make_async_remote_copy(
            src_ref=slab(target), dst_ref=windows.at[t, core],
            send_sem=a_send.at[j], recv_sem=a_recv.at[j],
            device_id=at_t(target), device_id_type=MESH,
        )

    def a_wait(j, source):
        pltpu.make_async_remote_copy(
            src_ref=slab(source), dst_ref=windows.at[source, core],
            send_sem=a_send.at[j], recv_sem=a_recv.at[j],
            device_id=at_t(source), device_id_type=MESH,
        ).wait_recv()

    def a_over(j, source, src):
        return pltpu.make_async_remote_copy(
            src_ref=src, dst_ref=windows.at[source, core],
            send_sem=a_pass.at[j], recv_sem=a_got.at[j],
            device_id=partner, device_id_type=MESH,
        )

    def a_over_wait(j, source):
        pltpu.make_async_remote_copy(
            src_ref=windows.at[source, 1 - core], dst_ref=windows.at[source, 1 - core],
            send_sem=a_pass.at[j], recv_sem=a_got.at[j],
            device_id=partner, device_id_type=MESH,
        ).wait_recv()

    mine = pltpu.make_async_copy(slab(t), windows.at[t, core], a_load)
    mine.start()

    def plane_ref(c, k, last, yy, xx):
        if k == 0:
            return held.at[c, k, yy] if last else held.at[c, k, yy, xx]
        if k == 1:
            return held.at[c, k, :, xx] if last else held.at[c, k, yy, xx]
        if not last:
            return held.at[c, k, yy, xx, z]
        return held.at[c, k, yy] if k == 2 else held.at[c, k, :, xx]

    def along_x(k, last):
        return (k in (0, 2)) != last

    def plane(c, k, last):
        ref = plane_ref(c, k, last, y, x)
        return pltpu.make_async_remote_copy(
            src_ref=ref, dst_ref=ref,
            send_sem=p_send.at[c, k, int(last)], recv_sem=p_recv.at[c, k, int(last)],
            device_id=at_t(tx if along_x(k, last) else ty), device_id_type=MESH,
        )

    def plane_wait(c, k, last):
        yy, xx = (y, 1 - x) if along_x(k, last) else (1 - y, x)
        ref = plane_ref(c, k, last, yy, xx)
        pltpu.make_async_remote_copy(
            src_ref=ref, dst_ref=ref,
            send_sem=p_send.at[c, k, int(last)], recv_sem=p_recv.at[c, k, int(last)],
            device_id=at_t(tx if along_x(k, last) else ty), device_id_type=MESH,
        ).wait_recv()

    def line_ref(c, g, source):
        if g == 0:
            return held.at[c, pl.ds(0, 2), y, x, source]
        return held.at[c, 2, y, :, source] if g == 1 else held.at[c, 3, :, x, source]

    def line(c, g, source, up):
        ref = line_ref(c, g, source)
        return pltpu.make_async_remote_copy(
            src_ref=ref, dst_ref=ref,
            send_sem=z_send.at[c, g, source, up], recv_sem=z_recv.at[c, g, source],
            device_id=(t, z + 1 if up else z - 1, core), device_id_type=MESH,
        )

    def both_ways(c, g):
        @pl.when(z < depth - 1)
        def _():
            line(c, g, z, 1).start()

        @pl.when(z > 0)
        def _():
            line(c, g, z, 0).start()

    def first(c, carry):
        for k in range(KINDS):
            own(c, k).wait()
        for k in (2, 3):
            plane(c, k, False).start()
        return carry

    def send_own(c):
        both_ways(c, 0)
        for k in (2, 3):
            plane_wait(c, k, False)
            both_ways(c, k - 1)

    def pass_on(c):
        for hop in range(1, depth):
            for g in range(3):
                @pl.when(z - hop >= 0)
                def _():
                    line(c, g, z - hop, 0).wait_recv()

                    @pl.when(z < depth - 1)
                    def _():
                        line(c, g, z - hop, 1).start()

                @pl.when(z + hop < depth)
                def _():
                    line(c, g, z + hop, 1).wait_recv()

                    @pl.when(z > 0)
                    def _():
                        line(c, g, z + hop, 0).start()
        for k in (0, 1):
            plane(c, k, False).start()
        for k in (2, 3):
            plane(c, k, True).start()

    def finish(c):
        for k in (0, 1):
            plane_wait(c, k, False)
            plane(c, k, True).start()

    def out_copy(c):
        return pltpu.make_async_copy(
            made.at[c], o_ref.at[:, pl.ds(pl.multiple_of(c * wide, LANES), wide)], o_sem.at[c]
        )

    def multiply(c):
        for k in range(KINDS):
            plane_wait(c, k, True)
        for k in range(0, KINDS, 2):
            pair = [held[c, k + i].reshape(-1, LANES) for i in range(2)]
            term = jnp.dot(
                left[...], jnp.concatenate(pair, axis=1), preferred_element_type=jnp.float32
            )
            made[c, :, k * LANES:(k + 2) * LANES] = term.astype(made.dtype)
        out_copy(c).start()

    first(0, 0)
    both_ways(0, 0)
    lax.fori_loop(1, chunks, first, 0)
    for j, target in enumerate((tx, ty, td)):
        a_copy(j, target).start()
    a_over(3, t, slab(t)).start()
    for k in (2, 3):
        plane_wait(0, k, False)
        both_ways(0, k - 1)

    def share():
        for j, source in enumerate((tx, ty, td)):
            a_wait(j, source)
            a_over(j, source, windows.at[source, core]).start()

    def turn():
        mine.wait()
        for j, source in enumerate((tx, ty, td, t)):
            a_over_wait(j, source)
        shift = pl.multiple_of((t * rows) % LANES, 16)
        piece = windows.shape[2]
        for j in range(windows.shape[0] * 2):
            turned[...] = windows[j // 2, j % 2].T
            left[:, j * piece:(j + 1) * piece] = turned[pl.ds(shift, rows), :]

    def step(i, carry):
        @pl.when(i + 1 < chunks)
        def _():
            send_own(i + 1)

        @pl.when(i < chunks)
        def _():
            pass_on(i)

        @pl.when(i == 0)
        def _():
            share()

        @pl.when(i == 1)
        def _():
            turn()

        @pl.when((i >= 1) & (i < chunks + 1))
        def _():
            finish(i - 1)

        @pl.when(i >= 2)
        def _():
            multiply(i - 2)

        return carry

    lax.fori_loop(0, chunks + 2, step, 0)

    for j, target in enumerate((tx, ty, td)):
        a_copy(j, target).wait_send()
        a_over(j, target, windows.at[target, core]).wait_send()
    a_over(3, t, slab(t)).wait_send()

    def drain(c, carry):
        for k in range(KINDS):
            for last in (False, True):
                plane(c, k, last).wait_send()
        for g in range(3):
            for source in range(depth):
                @pl.when((z < depth - 1) & (z >= source))
                def _():
                    line(c, g, source, 1).wait_send()

                @pl.when((z > 0) & (z <= source))
                def _():
                    line(c, g, source, 0).wait_send()
        out_copy(c).wait()
        return carry

    lax.fori_loop(0, chunks, drain, 0)


def gathered(shape, inputs, out_grad):
    depth = shape["din"]
    groups = shape["tok"]
    rows = inputs.shape[1] // groups
    window = max((j * rows) % LANES for j in range(groups)) + rows
    window = -(-window // LANES) * LANES
    piece = inputs.shape[0]
    tall, columns = out_grad.shape
    wide = KINDS * LANES
    chunks = columns // wide
    tokens = tall * depth * groups
    any_ref = pl.BlockSpec(memory_space=pl.ANY)
    dma = pltpu.SemaphoreType.DMA
    return pl.pallas_call(
        functools.partial(kernel, (depth, chunks, rows, window)),
        out_shape=jax.ShapeDtypeStruct((rows, columns), out_grad.dtype),
        in_specs=[pl.BlockSpec(memory_space=pltpu.HBM)] * 2,
        out_specs=any_ref,
        scratch_shapes=[
            pltpu.VMEM((chunks, KINDS, 2, 2, depth, tall, LANES), out_grad.dtype),
            pltpu.VMEM((groups, 2, piece, window), inputs.dtype),
            pltpu.VMEM((window, piece), inputs.dtype),
            pltpu.VMEM((rows, tokens), inputs.dtype),
            pltpu.VMEM((chunks, rows, wide), out_grad.dtype),
            dma((chunks, KINDS)),
            dma,
            dma((3,)),
            dma((3,)),
            dma((4,)),
            dma((4,)),
            dma((chunks, 3, depth, 2)),
            dma((chunks, 3, depth)),
            dma((chunks, KINDS, 2)),
            dma((chunks, KINDS, 2)),
            dma((chunks,)),
        ],
        compiler_params=pltpu.CompilerParams(
            collective_id=0, has_side_effects=True, vmem_limit_bytes=24 * 2**20
        ),
        cost_estimate=pl.CostEstimate(
            flops=2 * rows * tokens * columns,
            bytes_accessed=2 * rows * columns,
            transcendentals=0,
        ),
    )(inputs, out_grad)


def solution(mesh):
    shape = dict(mesh.shape)

    def local(inputs, out_grad):
        groups, depth = shape["tok"], shape["din"]
        rows = inputs.shape[1] // groups
        tall = out_grad.shape[0]
        spread = tall * (groups * depth - 1)
        summed = rows * (groups - 1) + tall * (depth - 1)
        fits = (
            groups == 4
            and shape["dout"] == 2
            and inputs.shape[0] == LANES
            and rows % 16 == 0
            and tall % 16 == 0
            and out_grad.shape[1] % (KINDS * LANES) == 0
        )
        if fits and spread < summed:
            return gathered(shape, inputs, out_grad)
        return scattered(inputs, out_grad)

    placed = (P(("tok", "dout"), "din"), P(("tok", "din"), "dout"))
    return jax.shard_map(
        local, mesh=mesh, in_specs=placed, out_specs=P(("din", "tok"), "dout"), check_vma=False
    )
```

```python
import functools

import jax
import jax.numpy as jnp
from jax import lax
from jax.experimental import pallas as pl
from jax.experimental.pallas import tpu as pltpu
from jax.sharding import PartitionSpec as P

MESH = pl.DeviceIdType.MESH
LANES = 128
KINDS = 4


def scattered(inputs, out_grad):
    gathered = lax.all_gather(inputs, "dout", axis=0, tiled=True)
    partial_term = lax.dot_general(
        gathered,
        lax.all_gather(out_grad, "din", axis=0, tiled=True),
        (((0,), (0,)), ((), ())),
        preferred_element_type=jnp.float32,
    )
    return lax.psum_scatter(
        partial_term.astype(jnp.bfloat16), "tok", scatter_dimension=0, tiled=True
    )


def kernel(sizes, a_ref, g_ref, o_ref, held, windows, turned, left, made,
           load_sem, a_load, a_send, a_recv, a_pass, a_got, z_send, z_recv, p_send, p_recv, o_sem):
    depth, chunks, rows, window = sizes
    t, z, core = lax.axis_index("tok"), lax.axis_index("din"), lax.axis_index("dout")
    y, x = t // 2, t % 2
    tx, ty = y * 2 + (1 - x), (1 - y) * 2 + x
    td = (1 - y) * 2 + (1 - x)
    wide = KINDS * LANES

    def at_t(other):
        return (other, z, core)

    partner = (t, z, 1 - core)

    def own(c, k):
        return pltpu.make_async_copy(
            g_ref.at[:, pl.ds(pl.multiple_of(c * wide + k * LANES, LANES), LANES)],
            held.at[c, k, y, x, z],
            load_sem.at[c, k],
        )

    def load(c, carry):
        for k in range(KINDS):
            own(c, k).start()
        return carry

    lax.fori_loop(0, chunks, load, 0)

    barrier = pltpu.get_barrier_semaphore()
    for other in (at_t(tx), at_t(ty), at_t(td), partner):
        pl.semaphore_signal(barrier, inc=1, device_id=other, device_id_type=MESH)

    @pl.when(z > 0)
    def _():
        pl.semaphore_signal(barrier, inc=1, device_id=(t, z - 1, core), device_id_type=MESH)

    @pl.when(z < depth - 1)
    def _():
        pl.semaphore_signal(barrier, inc=1, device_id=(t, z + 1, core), device_id_type=MESH)

    pl.semaphore_wait(barrier, 4 + jnp.where(z > 0, 1, 0) + jnp.where(z < depth - 1, 1, 0))

    def slab(owner):
        start = pl.multiple_of((owner * rows) // LANES * LANES, LANES)
        return a_ref.at[:, pl.ds(start, window)]

    def a_copy(j, target):
        return pltpu.make_async_remote_copy(
            src_ref=slab(target), dst_ref=windows.at[t, core],
            send_sem=a_send.at[j], recv_sem=a_recv.at[j],
            device_id=at_t(target), device_id_type=MESH,
        )

    def a_wait(j, source):
        pltpu.make_async_remote_copy(
            src_ref=slab(source), dst_ref=windows.at[source, core],
            send_sem=a_send.at[j], recv_sem=a_recv.at[j],
            device_id=at_t(source), device_id_type=MESH,
        ).wait_recv()

    def a_over(j, source, src):
        return pltpu.make_async_remote_copy(
            src_ref=src, dst_ref=windows.at[source, core],
            send_sem=a_pass.at[j], recv_sem=a_got.at[j],
            device_id=partner, device_id_type=MESH,
        )

    def a_over_wait(j, source):
        pltpu.make_async_remote_copy(
            src_ref=windows.at[source, 1 - core], dst_ref=windows.at[source, 1 - core],
            send_sem=a_pass.at[j], recv_sem=a_got.at[j],
            device_id=partner, device_id_type=MESH,
        ).wait_recv()

    mine = pltpu.make_async_copy(slab(t), windows.at[t, core], a_load)
    mine.start()

    def by_form(c, act):
        plain = (c > 0) & (c % 3 == 0)

        @pl.when(plain)
        def _():
            act(True)

        @pl.when(jnp.logical_not(plain))
        def _():
            act(False)

    def order_of(k, plain):
        return k + 2 if plain and k < 2 else k

    def early(plain):
        return [k for k in range(KINDS) if order_of(k, plain) < 2]

    def late(plain):
        return [k for k in range(KINDS) if order_of(k, plain) >= 2]

    def plane_ref(c, k, order, last, yy, xx):
        if order == 0:
            return held.at[c, k, yy] if last else held.at[c, k, yy, xx]
        if order == 1:
            return held.at[c, k, :, xx] if last else held.at[c, k, yy, xx]
        if not last:
            return held.at[c, k, yy, xx, z]
        return held.at[c, k, yy] if order == 2 else held.at[c, k, :, xx]

    def along_x(order, last):
        return (order in (0, 2)) != last

    def plane_to(c, k, order, last, ref):
        return pltpu.make_async_remote_copy(
            src_ref=ref, dst_ref=ref,
            send_sem=p_send.at[c, k, int(last)], recv_sem=p_recv.at[c, k, int(last)],
            device_id=at_t(tx if along_x(order, last) else ty), device_id_type=MESH,
        )

    def plane(c, k, plain, last):
        order = order_of(k, plain)
        return plane_to(c, k, order, last, plane_ref(c, k, order, last, y, x))

    def plane_wait(c, k, plain, last):
        order = order_of(k, plain)
        yy, xx = (y, 1 - x) if along_x(order, last) else (1 - y, x)
        plane_to(c, k, order, last, plane_ref(c, k, order, last, yy, xx)).wait_recv()

    def groups(plain):
        return late(plain) + ([] if plain else [0])

    def line_ref(c, g, plain, source):
        order = order_of(g, plain)
        if order == 0:
            return held.at[c, pl.ds(0, 2), y, x, source]
        return held.at[c, g, y, :, source] if order == 2 else held.at[c, g, :, x, source]

    def line(c, g, plain, source, up):
        ref = line_ref(c, g, plain, source)
        return pltpu.make_async_remote_copy(
            src_ref=ref, dst_ref=ref,
            send_sem=z_send.at[c, g, source, up], recv_sem=z_recv.at[c, g, source],
            device_id=(t, z + 1 if up else z - 1, core), device_id_type=MESH,
        )

    def both_ways(c, g, plain):
        @pl.when(z < depth - 1)
        def _():
            line(c, g, plain, z, 1).start()

        @pl.when(z > 0)
        def _():
            line(c, g, plain, z, 0).start()

    def first(c, carry):
        for k in range(KINDS):
            own(c, k).wait()

        def act(plain):
            for k in late(plain):
                plane(c, k, plain, False).start()

        by_form(c, act)
        return carry

    def send_early(c):
        def act(plain):
            if not plain:
                both_ways(c, 0, plain)

        by_form(c, act)

    def send_late(c):
        def act(plain):
            for k in late(plain):
                plane_wait(c, k, plain, False)
                both_ways(c, k, plain)

        by_form(c, act)

    def pass_on(c, hop):
        def act(plain):
            for g in sorted(groups(plain)):
                @pl.when(z - hop >= 0)
                def _():
                    line(c, g, plain, z - hop, 0).wait_recv()

                    @pl.when(z < depth - 1)
                    def _():
                        line(c, g, plain, z - hop, 1).start()

                @pl.when(z + hop < depth)
                def _():
                    line(c, g, plain, z + hop, 1).wait_recv()

                    @pl.when(z > 0)
                    def _():
                        line(c, g, plain, z + hop, 0).start()

        by_form(c, act)

    def spread(c):
        def act(plain):
            for k in early(plain):
                plane(c, k, plain, False).start()
            for k in late(plain):
                plane(c, k, plain, True).start()

        by_form(c, act)

    def finish(c):
        def act(plain):
            for k in early(plain):
                plane_wait(c, k, plain, False)
                plane(c, k, plain, True).start()

        by_form(c, act)

    def arrived(c):
        def act(plain):
            for k in range(KINDS):
                plane_wait(c, k, plain, True)

        by_form(c, act)

    def out_copy(c):
        return pltpu.make_async_copy(
            made.at[c], o_ref.at[:, pl.ds(pl.multiple_of(c * wide, LANES), wide)], o_sem.at[c]
        )

    def multiply(c):
        arrived(c)
        for k in range(0, KINDS, 2):
            pair = [held[c, k + i].reshape(-1, LANES) for i in range(2)]
            term = jnp.dot(
                left[...], jnp.concatenate(pair, axis=1), preferred_element_type=jnp.float32
            )
            made[c, :, k * LANES:(k + 2) * LANES] = term.astype(made.dtype)
        out_copy(c).start()

    first(0, 0)
    send_early(0)
    lax.fori_loop(1, chunks, first, 0)
    for j, target in enumerate((tx, ty, td)):
        a_copy(j, target).start()
    a_over(3, t, slab(t)).start()
    send_late(0)
    for c in range(1, depth - 1):
        for back in range(c):
            pass_on(back, c - back)
        send_early(c)
        send_late(c)

    def share():
        for j, source in enumerate((tx, ty, td)):
            a_wait(j, source)
            a_over(j, source, windows.at[source, core]).start()

    def turn():
        mine.wait()
        for j, source in enumerate((tx, ty, td, t)):
            a_over_wait(j, source)
        shift = pl.multiple_of((t * rows) % LANES, 16)
        piece = windows.shape[2]
        for j in range(windows.shape[0] * 2):
            turned[...] = windows[j // 2, j % 2].T
            left[:, j * piece:(j + 1) * piece] = turned[pl.ds(shift, rows), :]

    def step(i, carry):
        @pl.when(i < chunks)
        def _():
            pass_on(i, depth - 1)
            spread(i)

        for hop in range(depth - 2, 0, -1):
            ahead = depth - 1 - hop

            @pl.when(i + ahead < chunks)
            def _():
                pass_on(i + ahead, hop)

        @pl.when(i + depth - 1 < chunks)
        def _():
            send_early(i + depth - 1)
            send_late(i + depth - 1)

        @pl.when(i == 0)
        def _():
            share()

        @pl.when(i == 1)
        def _():
            turn()

        @pl.when((i >= 1) & (i < chunks + 1))
        def _():
            finish(i - 1)

        @pl.when(i >= 2)
        def _():
            multiply(i - 2)

        return carry

    lax.fori_loop(0, chunks + 2, step, 0)

    for j, target in enumerate((tx, ty, td)):
        a_copy(j, target).wait_send()
        a_over(j, target, windows.at[target, core]).wait_send()
    a_over(3, t, slab(t)).wait_send()

    def drain(c, carry):
        def act(plain):
            for k in range(KINDS):
                for last in (False, True):
                    plane(c, k, plain, last).wait_send()
            for g in groups(plain):
                for source in range(depth):
                    @pl.when((z < depth - 1) & (z >= source))
                    def _():
                        line(c, g, plain, source, 1).wait_send()

                    @pl.when((z > 0) & (z <= source))
                    def _():
                        line(c, g, plain, source, 0).wait_send()

        by_form(c, act)
        out_copy(c).wait()
        return carry

    lax.fori_loop(0, chunks, drain, 0)


def gathered(shape, inputs, out_grad):
    depth = shape["din"]
    groups = shape["tok"]
    rows = inputs.shape[1] // groups
    window = max((j * rows) % LANES for j in range(groups)) + rows
    window = -(-window // LANES) * LANES
    piece = inputs.shape[0]
    tall, columns = out_grad.shape
    wide = KINDS * LANES
    chunks = columns // wide
    tokens = tall * depth * groups
    any_ref = pl.BlockSpec(memory_space=pl.ANY)
    dma = pltpu.SemaphoreType.DMA
    return pl.pallas_call(
        functools.partial(kernel, (depth, chunks, rows, window)),
        out_shape=jax.ShapeDtypeStruct((rows, columns), out_grad.dtype),
        in_specs=[pl.BlockSpec(memory_space=pltpu.HBM)] * 2,
        out_specs=any_ref,
        scratch_shapes=[
            pltpu.VMEM((chunks, KINDS, 2, 2, depth, tall, LANES), out_grad.dtype),
            pltpu.VMEM((groups, 2, piece, window), inputs.dtype),
            pltpu.VMEM((window, piece), inputs.dtype),
            pltpu.VMEM((rows, tokens), inputs.dtype),
            pltpu.VMEM((chunks, rows, wide), out_grad.dtype),
            dma((chunks, KINDS)),
            dma,
            dma((3,)),
            dma((3,)),
            dma((4,)),
            dma((4,)),
            dma((chunks, KINDS, depth, 2)),
            dma((chunks, KINDS, depth)),
            dma((chunks, KINDS, 2)),
            dma((chunks, KINDS, 2)),
            dma((chunks,)),
        ],
        compiler_params=pltpu.CompilerParams(
            collective_id=0, has_side_effects=True, vmem_limit_bytes=24 * 2**20
        ),
        cost_estimate=pl.CostEstimate(
            flops=2 * rows * tokens * columns,
            bytes_accessed=2 * rows * columns,
            transcendentals=0,
        ),
    )(inputs, out_grad)


def solution(mesh):
    shape = dict(mesh.shape)

    def local(inputs, out_grad):
        groups, depth = shape["tok"], shape["din"]
        rows = inputs.shape[1] // groups
        tall = out_grad.shape[0]
        spread = tall * (groups * depth - 1)
        summed = rows * (groups - 1) + tall * (depth - 1)
        fits = (
            groups == 4
            and shape["dout"] == 2
            and inputs.shape[0] == LANES
            and rows % 16 == 0
            and tall % 16 == 0
            and out_grad.shape[1] % (KINDS * LANES) == 0
        )
        if fits and spread < summed:
            return gathered(shape, inputs, out_grad)
        return scattered(inputs, out_grad)

    placed = (P(("tok", "dout"), "din"), P(("tok", "din"), "dout"))
    return jax.shard_map(
        local, mesh=mesh, in_specs=placed, out_specs=P(("din", "tok"), "dout"), check_vma=False
    )
```
